32 devices in a mesh: dp: 4 (over y, core), tensor: 8 (over z, x).
Axes of the slice: x: 2, y: 2, z: 4, core: 2. Of those that a mesh axis runs over, the one named last changes fastest.
Arguments:
- grads: bfloat16 [4, 2, 7168, 2048], P('dp', None, 'tensor'), may hold values from -6 to 6
- master: float32 [2, 7168, 2048], P(None, 'dp', 'tensor'), may hold values from -0.0625 to 0.0625
- moment1: float32 [2, 7168, 2048], P(None, 'dp', 'tensor'), may hold values from -3 to 3
- moment2: float32 [2, 7168, 2048], P(None, 'dp', 'tensor'), may hold values from 1 to 30
- tokens: bfloat16 [1024, 7168], P('dp'), may hold values from -6 to 6
- route: int32 [512], P('dp'), may hold values from 0 to 255, as said below
Outputs:
- new_master: float32 [2, 7168, 2048], P(None, 'dp', 'tensor')
- new_moment1: float32 [2, 7168, 2048], P(None, 'dp', 'tensor')
- new_moment2: float32 [2, 7168, 2048], P(None, 'dp', 'tensor')
- rollout: bfloat16 [2, 7168, 2048], P(None, None, 'tensor')
- hidden: bfloat16 [512, 2048], P('dp', 'tensor')
The draws below stay inside these ranges and needn't reach their ends.
Inputs may be any that keep to these rules, and one draw needn't show every extreme that they name: route[i] indexes one of the 256 tokens of the data rank that holds routed row i; within one data rank's 128 routed rows no token appears twice.
All inputs are finite; a program needn't handle non-finite values.
Results may differ from the reference program's by a relative error of at most 0.019.
Values may be sent and summed in bfloat16 or wider, within the bound.
A program may use at most 128 MiB of HBM per device.

```python
import math
import jax
import jax.numpy as jnp
from jax import lax

D = 7168
H = 2048
TOK_DEV = 256
ROUTED_DEV = 128
TOKENS = 1024
ROUTED = 512
N_DP = 4


def draw_route(key, part):
    rank_keys = jax.random.split(key, ROUTED // ROUTED_DEV)

    def one_rank(rank_key):
        order = jax.random.permutation(rank_key, TOK_DEV)
        return order[:ROUTED_DEV]
    chosen = jax.vmap(one_rank)(rank_keys)
    return chosen.reshape(ROUTED).astype(jnp.int32)


def spiked(entries, key, source, target, parts, factor):
    owner, partner = [(jnp.arange(entries.shape[axis_at]) // (entries.shape[axis_at] // parts)).reshape([-1 if axis == axis_at else 1 for axis in range(entries.ndim)]) for axis_at in (source, target)]
    chosen = jax.random.permutation(key, parts)[partner]
    strong = (owner == chosen) | (owner == (partner + parts // 2) % parts)
    return jnp.where(strong, factor * entries, entries)


def shard_levels(stream_key, shape, cuts, least, largest):
    loudness = 1.0
    for axis_at, shards_of in cuts:
        draws = jax.random.uniform(jax.random.fold_in(jax.random.fold_in(stream_key, 6), axis_at), (shards_of,), jnp.float32, least / len(cuts), largest / len(cuts))
        loudness = loudness * jnp.repeat(jnp.exp(draws), shape[axis_at] // shards_of).reshape((-1,) + (1,) * (len(shape) - 1 - axis_at))
    return loudness


def centred(rng, dims, width, reach, shards=(), held_as=jnp.bfloat16):
    array = jax.random.normal(rng, dims, jnp.float32) * width
    if len(shards) > 0:
        array = shard_levels(rng, dims, shards, -0.22, 0.18) * array
    return jnp.clip(array, min=-reach, max=reach).astype(held_as)


def noise_with(stream_key, extent, deviation, limit, cuts, heavy, kind=jnp.bfloat16):
    values = deviation * jax.random.normal(stream_key, extent, jnp.float32)
    if cuts:
        values = values * shard_levels(stream_key, extent, cuts, -0.22, 0.18)
    return jnp.clip(spiked(values, jax.random.fold_in(stream_key, 3), *heavy), -limit, limit).astype(kind)


def setup_inputs(seed: int = 0) -> dict:
    key_list = jax.random.split(jax.random.key(seed), 7)
    grads = noise_with(key_list[0], (N_DP, 2, D, H), 1.0, 6.0, ((0, 4), (2, 8)), (0, 2, 4, 2.0))
    master = centred(key_list[1], (2, D, H), D ** -0.5, 0.0625, ((1, 4), (2, 8)), jnp.float32)
    moment1 = centred(key_list[2], (2, D, H), 0.5, 3.0, ((1, 4), (2, 8)), jnp.float32)
    moment2 = jnp.clip(jnp.exp(math.log(30.0) - 3.4011974 * jax.random.uniform(key_list[3], (2, D, H), jnp.float32) ** shard_levels(key_list[3], (2, D, H), ((1, 4), (2, 8)), -0.2, 0.2)), 1.0, 30.0)
    tokens = centred(key_list[4], (TOKENS, D), 1.0, 6.0, ((0, 4),))
    route = draw_route(jax.random.fold_in(key_list[6], 71), 0)
    return {"grads": grads, "master": master, "moment1": moment1, "moment2": moment2, "tokens": tokens, "route": route}


def reference(grads, master, moment1, moment2, tokens, route):

    def accumulate(carry, piece):
        return (carry + piece.astype(jnp.float32), None)
    start = jnp.zeros(master.shape, jnp.float32)
    grad_total, _ = lax.scan(accumulate, start, grads)
    new_moment1 = 0.9 * moment1 + 0.1 * grad_total
    new_moment2 = 0.95 * moment2 + 0.05 * grad_total * grad_total
    first_fix = 1.0 - 0.9 ** 10
    second_fix = 1.0 - 0.95 ** 10
    step_size = new_moment1 / first_fix / (jnp.sqrt(new_moment2 / second_fix) + 1e-08) + 0.1 * master
    new_master = master - 0.003 * step_size
    rollout = new_master.astype(jnp.bfloat16)
    block = jnp.arange(ROUTED, dtype=jnp.int32) // ROUTED_DEV
    row_index = (block * TOK_DEV + route).astype(jnp.int32)
    picked = jnp.take(tokens, row_index, axis=0)
    gate_out = jnp.dot(picked, rollout[0], preferred_element_type=jnp.float32)
    up_out = jnp.dot(picked, rollout[1], preferred_element_type=jnp.float32)
    hidden = (jax.nn.silu(gate_out) * up_out).astype(jnp.bfloat16)
    return (new_master, new_moment1, new_moment2, rollout, hidden)
```

```python
import functools

import jax
import jax.numpy as jnp
from jax import lax
from jax.experimental import pallas as pl
from jax.experimental.pallas import tpu as pltpu
from jax.sharding import PartitionSpec as P

MESH = pl.DeviceIdType.MESH
LANES = 128
CHUNK = 32
AHEAD = 4
LEAD = 3
LATE = 3
STRIP = 16


def body(grads, master, moment1, moment2, tokens, route):
    tensor_count = lax.axis_size("tensor")
    rank_count = lax.axis_size("dp")
    grad_local = grads[0]
    rows_tensor = grad_local.shape[1]
    hidden_width = grad_local.shape[2]
    col_width = hidden_width // tensor_count
    slab = rows_tensor // rank_count
    summed = lax.psum_scatter(grad_local, "dp", scatter_dimension=1, tiled=True).astype(jnp.float32)
    pieces = summed.reshape(2, slab, tensor_count, col_width)
    spread = lax.all_to_all(
        pieces.astype(jnp.bfloat16), "tensor", split_axis=2, concat_axis=1, tiled=True
    ).astype(pieces.dtype)
    spread = spread.reshape(2, rank_count, tensor_count // rank_count, slab, col_width)
    owned = lax.all_to_all(
        spread.astype(jnp.bfloat16), "dp", split_axis=1, concat_axis=3, tiled=True
    ).astype(spread.dtype)
    grad_total = owned.reshape(2, rows_tensor * tensor_count // rank_count, col_width)
    new_moment1 = 0.9 * moment1 + 0.1 * grad_total
    new_moment2 = 0.95 * moment2 + 0.05 * grad_total * grad_total
    first_fix = 1.0 - 0.9**10
    second_fix = 1.0 - 0.95**10
    step_size = (
        new_moment1 / first_fix / (jnp.sqrt(new_moment2 / second_fix) + 1e-08) + 0.1 * master
    )
    new_master = master - 0.003 * step_size
    rollout_shard = new_master.astype(jnp.bfloat16)
    replicated = lax.all_gather(rollout_shard, "dp", axis=1, tiled=True)
    picked = jnp.take(tokens, route, axis=0)
    both = jnp.einsum("rd,kdh->rkh", picked, replicated, preferred_element_type=jnp.float32)
    hidden = (jax.nn.silu(both[:, 0, :]) * both[:, 1, :]).astype(jnp.bfloat16)
    return (new_master, new_moment1, new_moment2, replicated, hidden)


def reduce_kernel(
    tensor_count,
    grads,
    state0,
    state1,
    state2,
    tokens,
    route,
    held0,
    held1,
    held2,
    roll,
    picked,
    mine,
    theirs,
    land,
    inward,
    token_rows,
    chosen,
    load_sem,
    swap_send,
    swap_recv,
    state_sem,
    token_sem,
    apart_send,
    same_send,
    land_recv,
    inward_send,
    inward_recv,
    cross_send,
    cross_recv,
    near_send,
    near_recv,
    far_send,
    far_recv,
    relay_send,
    relay_recv,
):
    states, held = (state0, state1, state2), (held0, held1, held2)
    rank = lax.axis_index("dp")
    place = lax.axis_index("tensor")
    row, core = rank // 2, rank % 2
    near = row * 2 + 1 - core
    far = (1 - row) * 2 + core
    subs = land.shape[1]
    slab = mine.shape[0]
    width = land.shape[4]
    chunk = CHUNK
    steps = slab // chunk
    owner, sub = place // subs, place % subs
    side, owner_core = owner // 2, owner % 2
    group = 2 * subs
    span = group * width
    home = row == side
    away = row != side
    same_cols = pl.ds(pl.multiple_of(side * span, span), span)
    apart_cols = pl.ds(pl.multiple_of((1 - side) * span, span), span)
    slot = jnp.where(home, 0, 1)

    def rows(step):
        return pl.ds(pl.multiple_of(step * chunk, chunk), chunk)

    def columns(goal):
        return pl.ds(pl.multiple_of(goal * width, width), width)

    def remote(source, target, send, recv, to_rank, to_place):
        return pltpu.make_async_remote_copy(
            src_ref=source,
            dst_ref=target,
            send_sem=send,
            recv_sem=recv,
            device_id=(to_rank, to_place),
            device_id_type=MESH,
        )

    def arrived(spot, sem):
        pltpu.make_async_copy(spot, spot, sem).wait()

    def load(step):
        return pltpu.make_async_copy(
            grads.at[0, core, rows(step)], mine.at[rows(step)], load_sem.at[step]
        )

    def swap(step):
        return remote(
            grads.at[0, 1 - core, rows(step)], theirs.at[rows(step)],
            swap_send.at[step], swap_recv.at[step], near, place,
        )

    def state(which, step):
        return pltpu.make_async_copy(
            states[which].at[:, :, rows(step)],
            held[which].at[:, :, rows(step)],
            state_sem.at[which * steps + step],
        )

    def inbound(step):
        return remote(
            mine.at[rows(step), same_cols], inward.at[rows(step)],
            inward_send.at[step], inward_recv.at[step], far, place,
        )

    def spread_apart(step, offset):
        goal = (1 - side) * group + (place + offset) % group
        return remote(
            mine.at[rows(step), columns(goal)],
            land.at[slot, sub, core, rows(step)],
            apart_send.at[step],
            land_recv.at[slot * steps + step],
            row * 2 + owner_core,
            goal,
        )

    def spread_same(step, offset):
        goal = side * group + (place + offset) % group
        return remote(
            mine.at[rows(step), columns(goal)],
            land.at[0, sub, core, rows(step)],
            same_send.at[step],
            land_recv.at[step],
            row * 2 + owner_core,
            goal,
        )

    def spread_self(step):
        return pltpu.make_async_copy(
            mine.at[rows(step), columns(place)],
            land.at[0, sub, core, rows(step)],
            land_recv.at[step],
        )

    def landed(step, part):
        arrived(land.at[part, :, :, rows(step)], land_recv.at[part * steps + step])

    def cross(step):
        return remote(
            land.at[1, :, :, rows(step)], land.at[1, :, :, rows(step)],
            cross_send.at[step], cross_recv.at[step], far, place,
        )

    def block(of_rank, step):
        return roll.at[:, pl.ds(of_rank * subs, subs), rows(step)]

    def to_near(of_rank, step):
        return remote(
            block(of_rank, step), block(of_rank, step),
            near_send.at[step], near_recv.at[step], near, place,
        )

    def to_far(of_rank, step):
        return remote(
            block(of_rank, step), block(of_rank, step),
            far_send.at[step], far_recv.at[step], far, place,
        )

    def relay(of_rank, step):
        return remote(
            block(of_rank, step), block(of_rank, step),
            relay_send.at[step], relay_recv.at[step], near, place,
        )

    def fetch(step):
        load(step).wait()
        swap(step).wait_recv()

    def combine(step, cols, third=None):
        @pl.loop(0, chunk // STRIP)
        def _(i):
            at = pl.ds(pl.multiple_of(step * chunk + i * STRIP, STRIP), STRIP)
            total = mine[at, cols].astype(jnp.float32) + theirs[at, cols].astype(jnp.float32)
            if third is not None:
                total = total + third[at].astype(jnp.float32)
            mine[at, cols] = total.astype(mine.dtype)

    def issue_inward(step):
        fetch(step)
        combine(step, same_cols)
        inbound(step).start()

    def issue_apart(step):
        combine(step, apart_cols)
        for offset in range(group):
            spread_apart(step, offset).start()

    def issue_same(step):
        inbound(step).wait_recv()
        combine(step, same_cols, inward)
        for offset in range(1, group):
            spread_same(step, offset).start()

        @pl.when(owner_core == core)
        def _():
            spread_self(step).start()

        @pl.when(owner_core != core)
        def _():
            spread_same(step, 0).start()

    first_fix = 1.0 - 0.9**10
    second_fix = 1.0 - 0.95**10

    def update(step, crossed):
        for which in range(3):
            state(which, step).wait()

        @pl.loop(0, chunk // STRIP)
        def _(i):
            at = pl.ds(pl.multiple_of(step * chunk + i * STRIP, STRIP), STRIP)
            for half in range(2):
                for piece in range(subs):
                    grad = land[0, piece, half, at].astype(jnp.float32)
                    if crossed:
                        grad = grad + land[1, piece, half, at].astype(jnp.float32)
                    old = held[0][half, piece, at]
                    moment1 = 0.9 * held[1][half, piece, at] + 0.1 * grad
                    moment2 = 0.95 * held[2][half, piece, at] + 0.05 * grad * grad
                    scaled = jnp.sqrt(moment2 * (1.0 / second_fix)) + 1e-08
                    change = moment1 * (1.0 / first_fix) / scaled + 0.1 * old
                    new = old - 0.003 * change
                    held[0][half, piece, at] = new
                    held[1][half, piece, at] = moment1
                    held[2][half, piece, at] = moment2
                    roll[half, rank * subs + piece, at] = new.astype(roll.dtype)

        to_far(rank, step).start()
        to_near(rank, step).start()

    barrier = pltpu.get_barrier_semaphore()
    peers = 0
    for hop in range(tensor_count):
        goal = (place + hop) % tensor_count
        for which in range(2):
            if hop or which:
                pl.semaphore_signal(
                    barrier, inc=1, device_id=(row * 2 + (core + which) % 2, goal), device_id_type=MESH
                )
                peers += 1
    pl.semaphore_signal(barrier, inc=1, device_id=(far, place), device_id_type=MESH)
    peers += 1

    token_copy = pltpu.make_async_copy(tokens, token_rows, token_sem)
    token_copy.start()

    @pl.loop(0, steps)
    def _(step):
        load(step).start()

    index = lax.broadcasted_iota(jnp.int32, (token_rows.shape[0], route.shape[1]), 0)
    onehot = jnp.where(index == route[...], 1.0, 0.0)
    chosen[...] = onehot.T.astype(chosen.dtype)
    token_copy.wait()
    wide = tensor_count * LANES

    @pl.loop(0, token_rows.shape[1] // wide)
    def _(part):
        at = pl.ds(pl.multiple_of(part * wide, wide), wide)
        some = jnp.dot(chosen[...], token_rows[:, at], preferred_element_type=jnp.float32)
        picked[:, at] = some.astype(picked.dtype)

    pl.semaphore_wait(barrier, peers)

    @pl.loop(0, steps)
    def _(step):
        swap(step).start()

    @pl.loop(0, steps)
    def _(step):
        for which in range(3):
            state(which, step).start()

    @pl.loop(0, AHEAD)
    def _(step):
        @pl.when(away)
        def _():
            issue_inward(step)

        @pl.when(home)
        def _():
            fetch(step)

        issue_apart(step)

    @pl.when(away)
    def _():
        @pl.loop(AHEAD, AHEAD + LEAD)
        def _(step):
            issue_inward(step)

    @pl.when(home)
    def _():
        @pl.loop(0, AHEAD)
        def _(step):
            issue_same(step)

    @pl.loop(0, steps + LATE)
    def _(now):
        @pl.when(home & (now < steps))
        def _():
            landed(now, 1)
            cross(now).start()

        @pl.when(home & (now < steps - AHEAD))
        def _():
            fetch(now + AHEAD)
            issue_apart(now + AHEAD)
            issue_same(now + AHEAD)

        @pl.when(away & (now < steps - AHEAD))
        def _():
            issue_apart(now + AHEAD)

        @pl.when(away & (now < steps - AHEAD - LEAD))
        def _():
            issue_inward(now + AHEAD + LEAD)

        @pl.when(home & (now < steps))
        def _():
            landed(now, 0)
            update(now, False)

        @pl.when(away & (now < steps))
        def _():
            landed(now, 0)
            cross(now).wait_recv()
            update(now, True)

        @pl.when(now >= LATE)
        def _():
            to_far(far, now - LATE).wait_recv()
            relay(far, now - LATE).start()

    @pl.loop(0, steps)
    def _(step):
        swap(step).wait_send()
        sent = mine.at[rows(step), apart_cols]
        arrived(sent, apart_send.at[step])

        @pl.when(away)
        def _():
            inbound(step).wait_send()

        @pl.when(home)
        def _():
            cross(step).wait_send()

        @pl.when(home & (owner_core == core))
        def _():
            part = mine.at[rows(step), pl.ds(0, span - width)]
            arrived(part, same_send.at[step])

        @pl.when(home & (owner_core != core))
        def _():
            part = mine.at[rows(step), pl.ds(0, span)]
            arrived(part, same_send.at[step])

        to_far(rank, step).wait_send()
        to_near(rank, step).wait_send()
        to_near(near, step).wait_recv()
        relay(far, step).wait_send()
        relay((1 - row) * 2 + 1 - core, step).wait_recv()


def finish_kernel(
    held0, held1, held2, roll, picked, out0, out1, out2, full, hidden, acc, small, sems
):
    copies = []
    for source, target in ((held0, out0), (held1, out1), (held2, out2), (roll, full)):
        for half in range(2):
            copies.append(
                pltpu.make_async_copy(source.at[half], target.at[half], sems.at[len(copies)])
            )
    for copy in copies:
        copy.start()
    acc[...] = jnp.zeros_like(acc)
    depth = picked.shape[1]
    wide = depth // 7 if depth % (7 * LANES) == 0 else LANES

    @pl.loop(0, depth // wide)
    def _(part):
        at = pl.ds(pl.multiple_of(part * wide, wide), wide)
        for half in range(2):
            acc[half] += jnp.dot(
                picked[:, at], roll[half, at], preferred_element_type=jnp.float32
            )

    gate, up = acc[0], acc[1]
    small[...] = (gate / (1.0 + jnp.exp(-gate)) * up).astype(small.dtype)
    last = pltpu.make_async_copy(small, hidden, sems.at[len(copies)])
    last.start()
    for copy in copies:
        copy.wait()
    last.wait()


def fused(grads, master, moment1, moment2, tokens, route):
    tensor_count = lax.axis_size("tensor")
    rank_count = lax.axis_size("dp")
    subs = tensor_count // rank_count
    slab, hidden_width = grads.shape[2:]
    width = hidden_width // tensor_count
    steps = slab // CHUNK
    routed = route.shape[0]
    depth = tokens.shape[1]
    split = (2, subs, slab, width)
    states = [array.reshape(split) for array in (master, moment1, moment2)]
    anywhere = pl.BlockSpec(memory_space=pl.ANY)
    vmem = pl.BlockSpec(memory_space=pltpu.VMEM)
    hbm = pl.BlockSpec(memory_space=pltpu.HBM)
    dma = pltpu.SemaphoreType.DMA
    half = jnp.bfloat16
    f32 = jnp.float32
    parts = pl.pallas_call(
        functools.partial(reduce_kernel, tensor_count),
        out_shape=[pltpu.VMEM(split, f32)] * 3
        + [
            pltpu.VMEM((2, tensor_count, slab, width), half),
            pltpu.VMEM((routed, depth), half),
        ],
        in_specs=[anywhere] * 5 + [vmem],
        out_specs=[vmem] * 5,
        scratch_shapes=[
            pltpu.VMEM((slab, hidden_width), half),
            pltpu.VMEM((slab, hidden_width), half),
            pltpu.VMEM((2, subs, 2, slab, width), half),
            pltpu.VMEM((slab, hidden_width // 2), half),
            pltpu.VMEM(tokens.shape, half),
            pltpu.VMEM((routed, tokens.shape[0]), half),
            dma((steps,)),
            dma((steps,)),
            dma((steps,)),
            dma((3 * steps,)),
            dma,
            dma((steps,)),
            dma((steps,)),
            dma((2 * steps,)),
        ]
        + [dma((steps,))] * 10,
        compiler_params=pltpu.CompilerParams(
            has_side_effects=True, collective_id=0, vmem_limit_bytes=42 * 1024 * 1024
        ),
    )(grads, *states, tokens, route.reshape(1, routed))
    whole = (2, subs * slab, width)
    wide = (2, tensor_count * slab, width)
    *held, roll, picked = parts
    held = [array.reshape(whole) for array in held]
    new_master, new1, new2, rollout, hidden = pl.pallas_call(
        finish_kernel,
        out_shape=[pltpu.HBM(whole, f32)] * 3
        + [pltpu.HBM(wide, half), pltpu.HBM((routed, width), half)],
        in_specs=[vmem] * 5,
        out_specs=[hbm] * 5,
        scratch_shapes=[
            pltpu.VMEM((2, routed, width), f32),
            pltpu.VMEM((routed, width), half),
            dma((9,)),
        ],
        compiler_params=pltpu.CompilerParams(vmem_limit_bytes=8 * 1024 * 1024),
    )(*held, roll.reshape(wide), picked)
    return (new_master, new1, new2, rollout, hidden)


def chosen_body(grads, master, moment1, moment2, tokens, route):
    tensor_count, rank_count = lax.axis_size("tensor"), lax.axis_size("dp")
    slab, hidden_width = grads.shape[2:]
    fits = (
        rank_count == 4
        and tensor_count % rank_count == 0
        and slab % LANES == 0
        and slab % CHUNK == 0
        and slab // CHUNK > AHEAD + LEAD
        and tokens.shape[1] % (tensor_count * LANES) == 0
        and hidden_width % (tensor_count * LANES) == 0
    )
    chosen = fused if fits else body
    return chosen(grads, master, moment1, moment2, tokens, route)


def solution(mesh):
    in_specs = (
        P("dp", None, "tensor", None),
        P(None, "dp", "tensor"),
        P(None, "dp", "tensor"),
        P(None, "dp", "tensor"),
        P("dp", None),
        P("dp"),
    )
    out_specs = (
        P(None, "dp", "tensor"),
        P(None, "dp", "tensor"),
        P(None, "dp", "tensor"),
        P(None, None, "tensor"),
        P("dp", "tensor"),
    )
    return jax.shard_map(chosen_body, mesh=mesh, in_specs=in_specs, out_specs=out_specs, check_vma=False)
```

```python
import functools

import jax
import jax.numpy as jnp
from jax import lax
from jax.experimental import pallas as pl
from jax.experimental.pallas import tpu as pltpu
from jax.sharding import PartitionSpec as P

MESH = pl.DeviceIdType.MESH
LANES = 128
CHUNK = 32
AHEAD = 3
SAME = 3
LEAD = 8
LATE = 4
PRE = 3
PICK = 4
STRIP = 16
SWAPS = (1, 2, 4, 8, 16)
READY = 4


def body(grads, master, moment1, moment2, tokens, route):
    tensor_count = lax.axis_size("tensor")
    rank_count = lax.axis_size("dp")
    grad_local = grads[0]
    rows_tensor = grad_local.shape[1]
    hidden_width = grad_local.shape[2]
    col_width = hidden_width // tensor_count
    slab = rows_tensor // rank_count
    summed = lax.psum_scatter(grad_local, "dp", scatter_dimension=1, tiled=True).astype(jnp.float32)
    pieces = summed.reshape(2, slab, tensor_count, col_width)
    spread = lax.all_to_all(
        pieces.astype(jnp.bfloat16), "tensor", split_axis=2, concat_axis=1, tiled=True
    ).astype(pieces.dtype)
    spread = spread.reshape(2, rank_count, tensor_count // rank_count, slab, col_width)
    owned = lax.all_to_all(
        spread.astype(jnp.bfloat16), "dp", split_axis=1, concat_axis=3, tiled=True
    ).astype(spread.dtype)
    grad_total = owned.reshape(2, rows_tensor * tensor_count // rank_count, col_width)
    new_moment1 = 0.9 * moment1 + 0.1 * grad_total
    new_moment2 = 0.95 * moment2 + 0.05 * grad_total * grad_total
    first_fix = 1.0 - 0.9**10
    second_fix = 1.0 - 0.95**10
    step_size = (
        new_moment1 / first_fix / (jnp.sqrt(new_moment2 / second_fix) + 1e-08) + 0.1 * master
    )
    new_master = master - 0.003 * step_size
    rollout_shard = new_master.astype(jnp.bfloat16)
    replicated = lax.all_gather(rollout_shard, "dp", axis=1, tiled=True)
    picked = jnp.take(tokens, route, axis=0)
    both = jnp.einsum("rd,kdh->rkh", picked, replicated, preferred_element_type=jnp.float32)
    hidden = (jax.nn.silu(both[:, 0, :]) * both[:, 1, :]).astype(jnp.bfloat16)
    return (new_master, new_moment1, new_moment2, replicated, hidden)


def reduce_kernel(
    tensor_count,
    grads,
    state0,
    state1,
    state2,
    tokens,
    route,
    held0,
    held1,
    held2,
    roll,
    picked,
    mine,
    theirs,
    leaving,
    land,
    inward,
    early,
    token_rows,
    chosen,
    load_sem,
    swap_send,
    swap_recv,
    state_sem,
    token_sem,
    apart_send,
    same_send,
    land_recv,
    inward_send,
    inward_recv,
    early_send,
    early_recv,
    cross_send,
    near_send,
    near_recv,
    far_send,
    far_recv,
    relay_send,
    relay_recv,
):
    states, held = (state0, state1, state2), (held0, held1, held2)
    rank = lax.axis_index("dp")
    place = lax.axis_index("tensor")
    row, core = rank // 2, rank % 2
    near = row * 2 + 1 - core
    far = (1 - row) * 2 + core
    across = (1 - row) * 2 + 1 - core
    subs = land.shape[1]
    slab = mine.shape[0]
    width = land.shape[4]
    chunk = CHUNK
    steps = slab // chunk
    owner, sub = place // subs, place % subs
    side, owner_core = owner // 2, owner % 2
    group = 2 * subs
    span = group * width
    home = row == side
    away = row != side
    same_cols = pl.ds(pl.multiple_of(side * span, span), span)
    apart_cols = pl.ds(pl.multiple_of((1 - side) * span, span), span)
    slot = jnp.where(home, 0, 1)

    def rows(step):
        return pl.ds(pl.multiple_of(step * chunk, chunk), chunk)

    def columns(goal):
        return pl.ds(pl.multiple_of(goal * width, width), width)

    def remote(source, target, send, recv, to_rank, to_place):
        return pltpu.make_async_remote_copy(
            src_ref=source,
            dst_ref=target,
            send_sem=send,
            recv_sem=recv,
            device_id=(to_rank, to_place),
            device_id_type=MESH,
        )

    def arrived(spot, sem):
        pltpu.make_async_copy(spot, spot, sem).wait()

    ready = READY * chunk
    stops = (*(stop for stop in SWAPS if stop < steps), steps)
    pieces = tuple(zip((0, *stops[:-1]), stops))
    late = steps - PRE
    kept = pl.ds(0, late * chunk)
    tail = pl.ds(late * chunk, PRE * chunk)

    def load(which):
        part = pl.ds(0, ready) if which == 0 else pl.ds(ready, slab - ready)
        return pltpu.make_async_copy(
            grads.at[0, core, part], mine.at[part], load_sem.at[which]
        )

    def bring():
        part = pl.ds(0, ready)
        return pltpu.make_async_copy(grads.at[0, 1 - core, part], leaving, load_sem.at[2])

    def swap(piece):
        start, stop = pieces[piece]
        part = pl.ds(start * chunk, (stop - start) * chunk)
        source = leaving.at[part] if stop <= READY else grads.at[0, 1 - core, part]
        return remote(source, theirs.at[part], swap_send, swap_recv.at[piece], near, place)

    def state(which):
        return pltpu.make_async_copy(states[which], held[which], state_sem.at[which])

    def inbound(step):
        return remote(
            mine.at[rows(step), same_cols], inward.at[rows(step)],
            inward_send, inward_recv.at[step], far, place,
        )

    def forward():
        return remote(
            mine.at[tail, apart_cols], early, early_send, early_recv, far, place
        )

    def spread_apart(step, offset):
        goal = (1 - side) * group + (place + offset) % group
        return remote(
            mine.at[rows(step), columns(goal)],
            land.at[slot, sub, core, rows(step)],
            apart_send,
            land_recv.at[slot * steps + step],
            row * 2 + owner_core,
            goal,
        )

    def spread_same(step, offset):
        goal = side * group + (place + offset) % group
        return remote(
            mine.at[rows(step), columns(goal)],
            land.at[0, sub, core, rows(step)],
            same_send,
            land_recv.at[step],
            row * 2 + owner_core,
            goal,
        )

    def spread_self(step):
        return pltpu.make_async_copy(
            mine.at[rows(step), columns(place)],
            land.at[0, sub, core, rows(step)],
            land_recv.at[step],
        )

    def landed(step, part):
        arrived(land.at[part, :, :, rows(step)], land_recv.at[part * steps + step])

    def cross(step):
        return remote(
            land.at[1, :, :, rows(step)], land.at[1, :, :, rows(step)],
            cross_send, land_recv.at[steps + step], far, place,
        )

    def block(of_rank, step):
        return roll.at[:, pl.ds(of_rank * subs, subs), rows(step)]

    def to_near(of_rank, step):
        return remote(
            block(of_rank, step), block(of_rank, step),
            near_send, near_recv, near, place,
        )

    def to_far(of_rank, step):
        return remote(
            block(of_rank, step), block(of_rank, step),
            far_send, far_recv.at[step], far, place,
        )

    def relay(of_rank, step):
        return remote(
            block(of_rank, step), block(of_rank, step),
            relay_send, relay_recv, near, place,
        )

    def combine(step, cols, third=None, base=0):
        @pl.loop(0, chunk // STRIP)
        def _(i):
            at = pl.ds(pl.multiple_of(step * chunk + i * STRIP, STRIP), STRIP)
            total = mine[at, cols].astype(jnp.float32) + theirs[at, cols].astype(jnp.float32)
            if third is not None:
                place_of = (step - base) * chunk + i * STRIP
                total = total + third[pl.ds(pl.multiple_of(place_of, STRIP), STRIP)].astype(
                    jnp.float32
                )
            mine[at, cols] = total.astype(mine.dtype)

    def issue_inward(step):
        combine(step, same_cols)
        inbound(step).start()

    def issue_apart(step):
        for offset in range(group):
            spread_apart(step, offset).start()

    def issue_same(step):
        inbound(step).wait_recv()
        combine(step, same_cols, inward)
        for offset in range(1, group):
            spread_same(step, offset).start()

        @pl.when(owner_core == core)
        def _():
            spread_self(step).start()

        @pl.when(owner_core != core)
        def _():
            spread_same(step, 0).start()

    def pass_on(step):
        to_far(far, step).wait_recv()
        relay(far, step).start()

    last = steps + LATE
    first_fix = 1.0 - 0.9**10
    second_fix = 1.0 - 0.95**10

    def update(step, crossed):
        @pl.loop(0, chunk // STRIP)
        def _(i):
            at = pl.ds(pl.multiple_of(step * chunk + i * STRIP, STRIP), STRIP)
            for half in range(2):
                for piece in range(subs):
                    grad = land[0, piece, half, at].astype(jnp.float32)
                    if crossed:
                        grad = grad + land[1, piece, half, at].astype(jnp.float32)
                    old = held[0][half, piece, at]
                    moment1 = 0.9 * held[1][half, piece, at] + 0.1 * grad
                    moment2 = 0.95 * held[2][half, piece, at] + 0.05 * grad * grad
                    scaled = jnp.sqrt(moment2 * (1.0 / second_fix)) + 1e-08
                    change = moment1 * (1.0 / first_fix) / scaled + 0.1 * old
                    new = old - 0.003 * change
                    held[0][half, piece, at] = new
                    held[1][half, piece, at] = moment1
                    held[2][half, piece, at] = moment2
                    roll[half, rank * subs + piece, at] = new.astype(roll.dtype)

        to_far(rank, step).start()
        to_near(rank, step).start()

    barrier = pltpu.get_barrier_semaphore()
    peers = 0
    for hop in range(tensor_count):
        goal = (place + hop) % tensor_count
        for which in range(2):
            if hop or which:
                pl.semaphore_signal(
                    barrier, inc=1, device_id=(row * 2 + (core + which) % 2, goal), device_id_type=MESH
                )
                peers += 1
    pl.semaphore_signal(barrier, inc=1, device_id=(far, place), device_id_type=MESH)
    peers += 1

    load(0).start()
    bring().start()
    load(1).start()
    for which in range(3):
        state(which).start()
    token_copy = pltpu.make_async_copy(tokens, token_rows, token_sem)
    token_copy.start()
    index = lax.broadcasted_iota(jnp.int32, (token_rows.shape[0], route.shape[1]), 0)
    onehot = jnp.where(index == route[...], 1.0, 0.0)
    chosen[...] = onehot.T.astype(chosen.dtype)
    wide = tensor_count * LANES
    picks = token_rows.shape[1] // wide

    def pick(part):
        at = pl.ds(pl.multiple_of(part * wide, wide), wide)
        some = jnp.dot(chosen[...], token_rows[:, at], preferred_element_type=jnp.float32)
        picked[:, at] = some.astype(picked.dtype)

    def pick_now(now):
        @pl.when(now == PICK)
        def _():
            token_copy.wait()

        @pl.when((now >= PICK) & (now < PICK + picks))
        def _():
            pick(now - PICK)

    load(0).wait()
    bring().wait()
    pl.semaphore_wait(barrier, peers)
    for piece in range(len(pieces)):
        swap(piece).start()

    def first(step, action):
        for piece, (start, _) in enumerate(pieces):
            if start == step:
                swap(piece).wait_recv()
        if step == READY:
            load(1).wait()
        action(step)

    def rest(begin):
        for piece, (start, _) in enumerate(pieces):
            if start >= begin:
                swap(piece).wait_recv()
        if begin <= READY:
            load(1).wait()
        for which in range(3):
            state(which).wait()

    def apart_plain(step):
        combine(step, apart_cols)
        issue_apart(step)

    @pl.when(home)
    def _():
        for step in range(AHEAD):
            first(step, apart_plain)
        rest(AHEAD)

        @pl.loop(0, SAME)
        def _(step):
            issue_same(step)

        @pl.loop(0, last)
        def _(now):
            @pl.when(now < late)
            def _():
                landed(now, 1)
                cross(now).start()

            @pl.when(now < late - AHEAD)
            def _():
                apart_plain(now + AHEAD)

            @pl.when(now == late - AHEAD)
            def _():
                forward().wait_recv()

            @pl.when((now >= late - AHEAD) & (now < steps - AHEAD))
            def _():
                combine(now + AHEAD, apart_cols, early, late)
                issue_apart(now + AHEAD)

            @pl.when(now < steps - SAME)
            def _():
                issue_same(now + SAME)

            @pl.when(now >= LATE)
            def _():
                pass_on(now - LATE)

            @pl.when(now < steps)
            def _():
                landed(now, 0)
                update(now, False)

            pick_now(now)

    @pl.when(away)
    def _():
        def both(step):
            issue_inward(step)
            apart_plain(step)

        for step in range(AHEAD):
            first(step, both)
        for step in range(AHEAD, LEAD):
            first(step, issue_inward)
        rest(LEAD)

        @pl.loop(late, steps)
        def _(step):
            combine(step, apart_cols)

        forward().start()

        @pl.loop(0, last)
        def _(now):
            @pl.when(now < late - AHEAD)
            def _():
                apart_plain(now + AHEAD)

            @pl.when(now < steps - LEAD)
            def _():
                issue_inward(now + LEAD)

            @pl.when(now < late)
            def _():
                landed(now, 0)
                cross(now).wait_recv()
                update(now, True)

            @pl.when((now >= late) & (now < steps))
            def _():
                landed(now, 0)
                update(now, False)

            @pl.when(now >= LATE)
            def _():
                pass_on(now - LATE)

            pick_now(now)

    arrived(theirs, swap_send)

    @pl.when(away)
    def _():
        arrived(mine.at[kept, apart_cols], apart_send)
        arrived(inward, inward_send)
        forward().wait_send()

    @pl.when(home)
    def _():
        arrived(mine.at[:, apart_cols], apart_send)
        arrived(land.at[1, :, :, kept], cross_send)

    @pl.when(home & (owner_core == core))
    def _():
        arrived(mine.at[:, pl.ds(0, span - width)], same_send)

    @pl.when(home & (owner_core != core))
    def _():
        arrived(mine.at[:, pl.ds(0, span)], same_send)

    own = roll.at[:, pl.ds(rank * subs, subs)]
    arrived(own, far_send)
    arrived(own, near_send)
    arrived(own, relay_send)
    arrived(roll.at[:, pl.ds(near * subs, subs)], near_recv)
    arrived(roll.at[:, pl.ds(across * subs, subs)], relay_recv)


def finish_kernel(
    held0, held1, held2, roll, picked, out0, out1, out2, full, hidden, acc, small, sems
):
    copies = []
    for source, target in ((held0, out0), (held1, out1), (held2, out2), (roll, full)):
        for half in range(2):
            copies.append(
                pltpu.make_async_copy(source.at[half], target.at[half], sems.at[len(copies)])
            )
    for copy in copies:
        copy.start()
    acc[...] = jnp.zeros_like(acc)
    depth = picked.shape[1]
    wide = depth // 7 if depth % (7 * LANES) == 0 else LANES

    @pl.loop(0, depth // wide)
    def _(part):
        at = pl.ds(pl.multiple_of(part * wide, wide), wide)
        for half in range(2):
            acc[half] += jnp.dot(
                picked[:, at], roll[half, at], preferred_element_type=jnp.float32
            )

    gate, up = acc[0], acc[1]
    small[...] = (gate / (1.0 + jnp.exp(-gate)) * up).astype(small.dtype)
    last = pltpu.make_async_copy(small, hidden, sems.at[len(copies)])
    last.start()
    for copy in copies:
        copy.wait()
    last.wait()


def fused(grads, master, moment1, moment2, tokens, route):
    tensor_count = lax.axis_size("tensor")
    rank_count = lax.axis_size("dp")
    subs = tensor_count // rank_count
    slab, hidden_width = grads.shape[2:]
    width = hidden_width // tensor_count
    steps = slab // CHUNK
    routed = route.shape[0]
    depth = tokens.shape[1]
    split = (2, subs, slab, width)
    states = [array.reshape(split) for array in (master, moment1, moment2)]
    anywhere = pl.BlockSpec(memory_space=pl.ANY)
    vmem = pl.BlockSpec(memory_space=pltpu.VMEM)
    hbm = pl.BlockSpec(memory_space=pltpu.HBM)
    dma = pltpu.SemaphoreType.DMA
    half = jnp.bfloat16
    f32 = jnp.float32
    parts = pl.pallas_call(
        functools.partial(reduce_kernel, tensor_count),
        out_shape=[pltpu.VMEM(split, f32)] * 3
        + [
            pltpu.VMEM((2, tensor_count, slab, width), half),
            pltpu.VMEM((routed, depth), half),
        ],
        in_specs=[anywhere] * 5 + [vmem],
        out_specs=[vmem] * 5,
        scratch_shapes=[
            pltpu.VMEM((slab, hidden_width), half),
            pltpu.VMEM((slab, hidden_width), half),
            pltpu.VMEM((READY * CHUNK, hidden_width), half),
            pltpu.VMEM((2, subs, 2, slab, width), half),
            pltpu.VMEM((slab, hidden_width // 2), half),
            pltpu.VMEM((PRE * CHUNK, hidden_width // 2), half),
            pltpu.VMEM(tokens.shape, half),
            pltpu.VMEM((routed, tokens.shape[0]), half),
            dma((3,)),
            dma,
            dma((len(SWAPS) + 1,)),
            dma((3,)),
            dma,
            dma,
            dma,
            dma((2 * steps,)),
            dma,
            dma((steps,)),
            dma,
            dma,
            dma,
            dma,
            dma,
            dma,
            dma((steps,)),
            dma,
            dma,
        ],
        compiler_params=pltpu.CompilerParams(
            has_side_effects=True, collective_id=0, vmem_limit_bytes=42 * 1024 * 1024
        ),
    )(grads, *states, tokens, route.reshape(1, routed))
    whole = (2, subs * slab, width)
    wide = (2, tensor_count * slab, width)
    *held, roll, picked = parts
    held = [array.reshape(whole) for array in held]
    new_master, new1, new2, rollout, hidden = pl.pallas_call(
        finish_kernel,
        out_shape=[pltpu.HBM(whole, f32)] * 3
        + [pltpu.HBM(wide, half), pltpu.HBM((routed, width), half)],
        in_specs=[vmem] * 5,
        out_specs=[hbm] * 5,
        scratch_shapes=[
            pltpu.VMEM((2, routed, width), f32),
            pltpu.VMEM((routed, width), half),
            dma((9,)),
        ],
        compiler_params=pltpu.CompilerParams(vmem_limit_bytes=8 * 1024 * 1024),
    )(*held, roll.reshape(wide), picked)
    return (new_master, new1, new2, rollout, hidden)


def chosen_body(grads, master, moment1, moment2, tokens, route):
    tensor_count, rank_count = lax.axis_size("tensor"), lax.axis_size("dp")
    slab, hidden_width = grads.shape[2:]
    fits = (
        rank_count == 4
        and tensor_count % rank_count == 0
        and slab % LANES == 0
        and slab % CHUNK == 0
        and slab // CHUNK > max(LEAD, *SWAPS, AHEAD + PRE)
        and tokens.shape[1] // (tensor_count * LANES) + PICK <= slab // CHUNK
        and tokens.shape[1] % (tensor_count * LANES) == 0
        and hidden_width % (tensor_count * LANES) == 0
    )
    chosen = fused if fits else body
    return chosen(grads, master, moment1, moment2, tokens, route)


def solution(mesh):
    in_specs = (
        P("dp", None, "tensor", None),
        P(None, "dp", "tensor"),
        P(None, "dp", "tensor"),
        P(None, "dp", "tensor"),
        P("dp", None),
        P("dp"),
    )
    out_specs = (
        P(None, "dp", "tensor"),
        P(None, "dp", "tensor"),
        P(None, "dp", "tensor"),
        P(None, None, "tensor"),
        P("dp", "tensor"),
    )
    return jax.shard_map(chosen_body, mesh=mesh, in_specs=in_specs, out_specs=out_specs, check_vma=False)
```

```python
import functools

import jax
import jax.numpy as jnp
from jax import lax
from jax.experimental import pallas as pl
from jax.experimental.pallas import tpu as pltpu
from jax.sharding import PartitionSpec as P

MESH = pl.DeviceIdType.MESH
LANES = 128
CHUNK = 32
AHEAD = 3
SAME = 3
LEAD = 8
LATE = 4
PRE = 3
PICK = 4
STRIP = 16
SWAPS = (1, 2, 4, 8, 16)
READY = 4


def body(grads, master, moment1, moment2, tokens, route):
    tensor_count = lax.axis_size("tensor")
    rank_count = lax.axis_size("dp")
    grad_local = grads[0]
    rows_tensor = grad_local.shape[1]
    hidden_width = grad_local.shape[2]
    col_width = hidden_width // tensor_count
    slab = rows_tensor // rank_count
    summed = lax.psum_scatter(grad_local, "dp", scatter_dimension=1, tiled=True).astype(jnp.float32)
    pieces = summed.reshape(2, slab, tensor_count, col_width)
    spread = lax.all_to_all(
        pieces.astype(jnp.bfloat16), "tensor", split_axis=2, concat_axis=1, tiled=True
    ).astype(pieces.dtype)
    spread = spread.reshape(2, rank_count, tensor_count // rank_count, slab, col_width)
    owned = lax.all_to_all(
        spread.astype(jnp.bfloat16), "dp", split_axis=1, concat_axis=3, tiled=True
    ).astype(spread.dtype)
    grad_total = owned.reshape(2, rows_tensor * tensor_count // rank_count, col_width)
    new_moment1 = 0.9 * moment1 + 0.1 * grad_total
    new_moment2 = 0.95 * moment2 + 0.05 * grad_total * grad_total
    first_fix = 1.0 - 0.9**10
    second_fix = 1.0 - 0.95**10
    step_size = (
        new_moment1 / first_fix / (jnp.sqrt(new_moment2 / second_fix) + 1e-08) + 0.1 * master
    )
    new_master = master - 0.003 * step_size
    rollout_shard = new_master.astype(jnp.bfloat16)
    replicated = lax.all_gather(rollout_shard, "dp", axis=1, tiled=True)
    picked = jnp.take(tokens, route, axis=0)
    both = jnp.einsum("rd,kdh->rkh", picked, replicated, preferred_element_type=jnp.float32)
    hidden = (jax.nn.silu(both[:, 0, :]) * both[:, 1, :]).astype(jnp.bfloat16)
    return (new_master, new_moment1, new_moment2, replicated, hidden)


def reduce_kernel(
    tensor_count,
    grads,
    state0,
    state1,
    state2,
    tokens,
    route,
    held0,
    held1,
    held2,
    roll,
    picked,
    mine,
    theirs,
    leaving,
    land,
    inward,
    early,
    token_rows,
    chosen,
    table,
    load_sem,
    swap_send,
    swap_recv,
    state_sem,
    token_sem,
    table_sem,
    apart_send,
    same_send,
    land_recv,
    inward_send,
    inward_recv,
    early_send,
    early_recv,
    cross_send,
    near_send,
    near_recv,
    far_send,
    far_recv,
    relay_send,
    relay_recv,
):
    states, held = (state0, state1, state2), (held0, held1, held2)
    rank = lax.axis_index("dp")
    place = lax.axis_index("tensor")
    row, core = rank // 2, rank % 2
    near = row * 2 + 1 - core
    far = (1 - row) * 2 + core
    across = (1 - row) * 2 + 1 - core
    subs = land.shape[1]
    slab = mine.shape[0]
    width = land.shape[4]
    chunk = CHUNK
    steps = slab // chunk
    owner, sub = place // subs, place % subs
    side, owner_core = owner // 2, owner % 2
    group = 2 * subs
    span = group * width
    home = row == side
    away = row != side
    same_cols = pl.ds(pl.multiple_of(side * span, span), span)
    apart_cols = pl.ds(pl.multiple_of((1 - side) * span, span), span)
    slot = jnp.where(home, 0, 1)

    def rows(step):
        return pl.ds(pl.multiple_of(step * chunk, chunk), chunk)

    def columns(goal):
        return pl.ds(pl.multiple_of(goal * width, width), width)

    def remote(source, target, send, recv, to_rank, to_place):
        return pltpu.make_async_remote_copy(
            src_ref=source,
            dst_ref=target,
            send_sem=send,
            recv_sem=recv,
            device_id=(to_rank, to_place),
            device_id_type=MESH,
        )

    def arrived(spot, sem):
        pltpu.make_async_copy(spot, spot, sem).wait()

    ready = READY * chunk
    stops = (*(stop for stop in SWAPS if stop < steps), steps)
    pieces = tuple(zip((0, *stops[:-1]), stops))
    late = steps - PRE
    kept = pl.ds(0, late * chunk)
    tail = pl.ds(late * chunk, PRE * chunk)

    def load(which):
        part = pl.ds(0, ready) if which == 0 else pl.ds(ready, slab - ready)
        return pltpu.make_async_copy(
            grads.at[0, core, part], mine.at[part], load_sem.at[which]
        )

    def bring():
        part = pl.ds(0, ready)
        return pltpu.make_async_copy(grads.at[0, 1 - core, part], leaving, load_sem.at[2])

    def swap(piece):
        start, stop = pieces[piece]
        part = pl.ds(start * chunk, (stop - start) * chunk)
        source = leaving.at[part] if stop <= READY else grads.at[0, 1 - core, part]
        return remote(source, theirs.at[part], swap_send, swap_recv.at[piece], near, place)

    def state(which):
        return pltpu.make_async_copy(states[which], held[which], state_sem.at[which])

    def inbound(step):
        return remote(
            mine.at[rows(step), same_cols], inward.at[rows(step)],
            inward_send, inward_recv.at[step], far, place,
        )

    def forward():
        return remote(
            mine.at[tail, apart_cols], early, early_send, early_recv, far, place
        )

    def spread_apart(step, offset):
        goal = (1 - side) * group + (place + offset) % group
        return remote(
            mine.at[rows(step), columns(goal)],
            land.at[slot, sub, core, rows(step)],
            apart_send,
            land_recv.at[slot * steps + step],
            row * 2 + owner_core,
            goal,
        )

    def spread_same(step, offset):
        goal = side * group + (place + offset) % group
        return remote(
            mine.at[rows(step), columns(goal)],
            land.at[0, sub, core, rows(step)],
            same_send,
            land_recv.at[step],
            row * 2 + owner_core,
            goal,
        )

    def spread_self(step):
        return pltpu.make_async_copy(
            mine.at[rows(step), columns(place)],
            land.at[0, sub, core, rows(step)],
            land_recv.at[step],
        )

    def landed(step, part):
        arrived(land.at[part, :, :, rows(step)], land_recv.at[part * steps + step])

    def cross(step):
        return remote(
            land.at[1, :, :, rows(step)], land.at[1, :, :, rows(step)],
            cross_send, land_recv.at[steps + step], far, place,
        )

    def block(of_rank, step):
        return roll.at[:, pl.ds(of_rank * subs, subs), rows(step)]

    def to_near(of_rank, step):
        return remote(
            block(of_rank, step), block(of_rank, step),
            near_send, near_recv, near, place,
        )

    def to_far(of_rank, step):
        return remote(
            block(of_rank, step), block(of_rank, step),
            far_send, far_recv.at[step], far, place,
        )

    def relay(of_rank, step):
        return remote(
            block(of_rank, step), block(of_rank, step),
            relay_send, relay_recv, near, place,
        )

    def combine(step, cols, third=None, base=0):
        @pl.loop(0, chunk // STRIP)
        def _(i):
            at = pl.ds(pl.multiple_of(step * chunk + i * STRIP, STRIP), STRIP)
            total = mine[at, cols].astype(jnp.float32) + theirs[at, cols].astype(jnp.float32)
            if third is not None:
                place_of = (step - base) * chunk + i * STRIP
                total = total + third[pl.ds(pl.multiple_of(place_of, STRIP), STRIP)].astype(
                    jnp.float32
                )
            mine[at, cols] = total.astype(mine.dtype)

    def issue_inward(step):
        combine(step, same_cols)
        inbound(step).start()

    def issue_apart(step):
        for offset in range(group):
            spread_apart(step, offset).start()

    def issue_same(step):
        inbound(step).wait_recv()
        combine(step, same_cols, inward)
        for offset in range(1, group):
            spread_same(step, offset).start()

        @pl.when(owner_core == core)
        def _():
            spread_self(step).start()

        @pl.when(owner_core != core)
        def _():
            spread_same(step, 0).start()

    def pass_on(step):
        to_far(far, step).wait_recv()
        relay(far, step).start()

    last = steps + LATE
    first_fix = 1.0 - 0.9**10
    second_fix = 1.0 - 0.95**10

    def update(step, crossed):
        @pl.loop(0, chunk // STRIP)
        def _(i):
            at = pl.ds(pl.multiple_of(step * chunk + i * STRIP, STRIP), STRIP)
            for half in range(2):
                for piece in range(subs):
                    grad = land[0, piece, half, at].astype(jnp.float32)
                    if crossed:
                        grad = grad + land[1, piece, half, at].astype(jnp.float32)
                    old = held[0][half, piece, at]
                    moment1 = 0.9 * held[1][half, piece, at] + 0.1 * grad
                    moment2 = 0.95 * held[2][half, piece, at] + 0.05 * grad * grad
                    scaled = jnp.sqrt(moment2 * (1.0 / second_fix)) + 1e-08
                    change = moment1 * (1.0 / first_fix) / scaled + 0.1 * old
                    new = old - 0.003 * change
                    held[0][half, piece, at] = new
                    held[1][half, piece, at] = moment1
                    held[2][half, piece, at] = moment2
                    roll[half, rank * subs + piece, at] = new.astype(roll.dtype)

        to_far(rank, step).start()
        to_near(rank, step).start()

    barrier = pltpu.get_barrier_semaphore()
    peers = 0
    for hop in range(tensor_count):
        goal = (place + hop) % tensor_count
        for which in range(2):
            if hop or which:
                pl.semaphore_signal(
                    barrier, inc=1, device_id=(row * 2 + (core + which) % 2, goal), device_id_type=MESH
                )
                peers += 1
    pl.semaphore_signal(barrier, inc=1, device_id=(far, place), device_id_type=MESH)
    peers += 1

    load(0).start()
    bring().start()
    token_copy = pltpu.make_async_copy(tokens, token_rows, token_sem)
    table_copy = pltpu.make_async_copy(route, table, table_sem)
    table_copy.start()
    wide = tensor_count * LANES
    picks = token_rows.shape[1] // wide

    def pick(part):
        at = pl.ds(pl.multiple_of(part * wide, wide), wide)
        some = jnp.dot(chosen[...], token_rows[:, at], preferred_element_type=jnp.float32)
        picked[:, at] = some.astype(picked.dtype)

    def pick_now(now):
        @pl.when(now == PICK)
        def _():
            token_copy.wait()
            table_copy.wait()
            index = lax.broadcasted_iota(jnp.int32, (token_rows.shape[0], table.shape[1]), 0)
            onehot = jnp.where(index == table[...], 1.0, 0.0)
            chosen[...] = onehot.T.astype(chosen.dtype)

        @pl.when((now >= PICK) & (now < PICK + picks))
        def _():
            pick(now - PICK)

    load(0).wait()
    bring().wait()
    pl.semaphore_wait(barrier, peers)
    for piece in range(len(pieces)):
        swap(piece).start()
    load(1).start()
    for which in range(3):
        state(which).start()
    token_copy.start()

    def first(step, action):
        for piece, (start, _) in enumerate(pieces):
            if start == step:
                swap(piece).wait_recv()
        if step == READY:
            load(1).wait()
        action(step)

    def rest(begin):
        for piece, (start, _) in enumerate(pieces):
            if start >= begin:
                swap(piece).wait_recv()
        if begin <= READY:
            load(1).wait()
        for which in range(3):
            state(which).wait()

    def apart_plain(step):
        combine(step, apart_cols)
        issue_apart(step)

    @pl.when(home)
    def _():
        for step in range(AHEAD):
            first(step, apart_plain)
        for step in range(SAME):
            issue_same(step)
        rest(AHEAD)

        @pl.loop(0, last)
        def _(now):
            @pl.when(now < late)
            def _():
                landed(now, 1)
                cross(now).start()

            @pl.when(now < late - AHEAD)
            def _():
                apart_plain(now + AHEAD)

            @pl.when(now == late - AHEAD)
            def _():
                forward().wait_recv()

            @pl.when((now >= late - AHEAD) & (now < steps - AHEAD))
            def _():
                combine(now + AHEAD, apart_cols, early, late)
                issue_apart(now + AHEAD)

            @pl.when(now < steps - SAME)
            def _():
                issue_same(now + SAME)

            @pl.when(now >= LATE)
            def _():
                pass_on(now - LATE)

            @pl.when(now < steps)
            def _():
                landed(now, 0)
                update(now, False)

            pick_now(now)

    @pl.when(away)
    def _():
        def both(step):
            issue_inward(step)
            apart_plain(step)

        for step in range(AHEAD):
            first(step, both)
        for step in range(AHEAD, LEAD):
            first(step, issue_inward)
        rest(LEAD)

        @pl.loop(late, steps)
        def _(step):
            combine(step, apart_cols)

        forward().start()

        @pl.loop(0, last)
        def _(now):
            @pl.when(now < late - AHEAD)
            def _():
                apart_plain(now + AHEAD)

            @pl.when(now < steps - LEAD)
            def _():
                issue_inward(now + LEAD)

            @pl.when(now < late)
            def _():
                landed(now, 0)
                cross(now).wait_recv()
                update(now, True)

            @pl.when((now >= late) & (now < steps))
            def _():
                landed(now, 0)
                update(now, False)

            @pl.when(now >= LATE)
            def _():
                pass_on(now - LATE)

            pick_now(now)

    arrived(theirs, swap_send)

    @pl.when(away)
    def _():
        arrived(mine.at[kept, apart_cols], apart_send)
        arrived(inward, inward_send)
        forward().wait_send()

    @pl.when(home)
    def _():
        arrived(mine.at[:, apart_cols], apart_send)
        arrived(land.at[1, :, :, kept], cross_send)

    @pl.when(home & (owner_core == core))
    def _():
        arrived(mine.at[:, pl.ds(0, span - width)], same_send)

    @pl.when(home & (owner_core != core))
    def _():
        arrived(mine.at[:, pl.ds(0, span)], same_send)

    own = roll.at[:, pl.ds(rank * subs, subs)]
    arrived(own, far_send)
    arrived(own, near_send)
    arrived(own, relay_send)
    arrived(roll.at[:, pl.ds(near * subs, subs)], near_recv)
    arrived(roll.at[:, pl.ds(across * subs, subs)], relay_recv)


def finish_kernel(
    held0, held1, held2, roll, picked, out0, out1, out2, full, hidden, acc, small, sems
):
    copies = []
    for source, target in ((held0, out0), (held1, out1), (held2, out2), (roll, full)):
        for half in range(2):
            copies.append(
                pltpu.make_async_copy(source.at[half], target.at[half], sems.at[len(copies)])
            )
    for copy in copies:
        copy.start()
    acc[...] = jnp.zeros_like(acc)
    depth = picked.shape[1]
    wide = depth // 7 if depth % (7 * LANES) == 0 else LANES

    @pl.loop(0, depth // wide)
    def _(part):
        at = pl.ds(pl.multiple_of(part * wide, wide), wide)
        for half in range(2):
            acc[half] += jnp.dot(
                picked[:, at], roll[half, at], preferred_element_type=jnp.float32
            )

    gate, up = acc[0], acc[1]
    small[...] = (gate / (1.0 + jnp.exp(-gate)) * up).astype(small.dtype)
    last = pltpu.make_async_copy(small, hidden, sems.at[len(copies)])
    last.start()
    for copy in copies:
        copy.wait()
    last.wait()


def fused(grads, master, moment1, moment2, tokens, route):
    tensor_count = lax.axis_size("tensor")
    rank_count = lax.axis_size("dp")
    subs = tensor_count // rank_count
    slab, hidden_width = grads.shape[2:]
    width = hidden_width // tensor_count
    steps = slab // CHUNK
    routed = route.shape[0]
    depth = tokens.shape[1]
    split = (2, subs, slab, width)
    states = [array.reshape(split) for array in (master, moment1, moment2)]
    anywhere = pl.BlockSpec(memory_space=pl.ANY)
    vmem = pl.BlockSpec(memory_space=pltpu.VMEM)
    hbm = pl.BlockSpec(memory_space=pltpu.HBM)
    dma = pltpu.SemaphoreType.DMA
    half = jnp.bfloat16
    f32 = jnp.float32
    parts = pl.pallas_call(
        functools.partial(reduce_kernel, tensor_count),
        out_shape=[pltpu.VMEM(split, f32)] * 3
        + [
            pltpu.VMEM((2, tensor_count, slab, width), half),
            pltpu.VMEM((routed, depth), half),
        ],
        in_specs=[anywhere] * 6,
        out_specs=[vmem] * 5,
        scratch_shapes=[
            pltpu.VMEM((slab, hidden_width), half),
            pltpu.VMEM((slab, hidden_width), half),
            pltpu.VMEM((READY * CHUNK, hidden_width), half),
            pltpu.VMEM((2, subs, 2, slab, width), half),
            pltpu.VMEM((slab, hidden_width // 2), half),
            pltpu.VMEM((PRE * CHUNK, hidden_width // 2), half),
            pltpu.VMEM(tokens.shape, half),
            pltpu.VMEM((routed, tokens.shape[0]), half),
            pltpu.VMEM((1, routed), jnp.int32),
            dma((3,)),
            dma,
            dma((len(SWAPS) + 1,)),
            dma((3,)),
            dma,
            dma,
            dma,
            dma,
            dma((2 * steps,)),
            dma,
            dma((steps,)),
            dma,
            dma,
            dma,
            dma,
            dma,
            dma,
            dma((steps,)),
            dma,
            dma,
        ],
        compiler_params=pltpu.CompilerParams(
            has_side_effects=True, collective_id=0, vmem_limit_bytes=42 * 1024 * 1024
        ),
    )(grads, *states, tokens, route.reshape(1, routed))
    whole = (2, subs * slab, width)
    wide = (2, tensor_count * slab, width)
    *held, roll, picked = parts
    held = [array.reshape(whole) for array in held]
    new_master, new1, new2, rollout, hidden = pl.pallas_call(
        finish_kernel,
        out_shape=[pltpu.HBM(whole, f32)] * 3
        + [pltpu.HBM(wide, half), pltpu.HBM((routed, width), half)],
        in_specs=[vmem] * 5,
        out_specs=[hbm] * 5,
        scratch_shapes=[
            pltpu.VMEM((2, routed, width), f32),
            pltpu.VMEM((routed, width), half),
            dma((9,)),
        ],
        compiler_params=pltpu.CompilerParams(vmem_limit_bytes=8 * 1024 * 1024),
    )(*held, roll.reshape(wide), picked)
    return (new_master, new1, new2, rollout, hidden)


def chosen_body(grads, master, moment1, moment2, tokens, route):
    tensor_count, rank_count = lax.axis_size("tensor"), lax.axis_size("dp")
    slab, hidden_width = grads.shape[2:]
    fits = (
        rank_count == 4
        and tensor_count % rank_count == 0
        and slab % LANES == 0
        and slab % CHUNK == 0
        and slab // CHUNK > max(LEAD, *SWAPS, AHEAD + PRE)
        and tokens.shape[1] // (tensor_count * LANES) + PICK <= slab // CHUNK
        and tokens.shape[1] % (tensor_count * LANES) == 0
        and hidden_width % (tensor_count * LANES) == 0
    )
    chosen = fused if fits else body
    return chosen(grads, master, moment1, moment2, tokens, route)


def solution(mesh):
    in_specs = (
        P("dp", None, "tensor", None),
        P(None, "dp", "tensor"),
        P(None, "dp", "tensor"),
        P(None, "dp", "tensor"),
        P("dp", None),
        P("dp"),
    )
    out_specs = (
        P(None, "dp", "tensor"),
        P(None, "dp", "tensor"),
        P(None, "dp", "tensor"),
        P(None, None, "tensor"),
        P("dp", "tensor"),
    )
    return jax.shard_map(chosen_body, mesh=mesh, in_specs=in_specs, out_specs=out_specs, check_vma=False)
```

```python
import functools

import jax
import jax.numpy as jnp
from jax import lax
from jax.experimental import pallas as pl
from jax.experimental.pallas import tpu as pltpu
from jax.sharding import PartitionSpec as P

MESH = pl.DeviceIdType.MESH
LANES = 128
CHUNK = 32
AHEAD = 3
SAME = 3
LEAD = 8
LATE = 4
PRE = 3
PICK = 4
STRIP = 16
SWAPS = (1, 2, 4, 8, 16)
READY = 4


def body(grads, master, moment1, moment2, tokens, route):
    tensor_count = lax.axis_size("tensor")
    rank_count = lax.axis_size("dp")
    grad_local = grads[0]
    rows_tensor = grad_local.shape[1]
    hidden_width = grad_local.shape[2]
    col_width = hidden_width // tensor_count
    slab = rows_tensor // rank_count
    summed = lax.psum_scatter(grad_local, "dp", scatter_dimension=1, tiled=True).astype(jnp.float32)
    pieces = summed.reshape(2, slab, tensor_count, col_width)
    spread = lax.all_to_all(
        pieces.astype(jnp.bfloat16), "tensor", split_axis=2, concat_axis=1, tiled=True
    ).astype(pieces.dtype)
    spread = spread.reshape(2, rank_count, tensor_count // rank_count, slab, col_width)
    owned = lax.all_to_all(
        spread.astype(jnp.bfloat16), "dp", split_axis=1, concat_axis=3, tiled=True
    ).astype(spread.dtype)
    grad_total = owned.reshape(2, rows_tensor * tensor_count // rank_count, col_width)
    new_moment1 = 0.9 * moment1 + 0.1 * grad_total
    new_moment2 = 0.95 * moment2 + 0.05 * grad_total * grad_total
    first_fix = 1.0 - 0.9**10
    second_fix = 1.0 - 0.95**10
    step_size = (
        new_moment1 / first_fix / (jnp.sqrt(new_moment2 / second_fix) + 1e-08) + 0.1 * master
    )
    new_master = master - 0.003 * step_size
    rollout_shard = new_master.astype(jnp.bfloat16)
    replicated = lax.all_gather(rollout_shard, "dp", axis=1, tiled=True)
    picked = jnp.take(tokens, route, axis=0)
    both = jnp.einsum("rd,kdh->rkh", picked, replicated, preferred_element_type=jnp.float32)
    hidden = (jax.nn.silu(both[:, 0, :]) * both[:, 1, :]).astype(jnp.bfloat16)
    return (new_master, new_moment1, new_moment2, replicated, hidden)


def reduce_kernel(
    tensor_count,
    grads,
    state0,
    state1,
    state2,
    tokens,
    route,
    held0,
    held1,
    held2,
    roll,
    picked,
    mine,
    theirs,
    leaving,
    land,
    inward,
    early,
    token_rows,
    chosen,
    table,
    load_sem,
    swap_send,
    swap_recv,
    state_sem,
    token_sem,
    table_sem,
    apart_send,
    same_send,
    land_recv,
    inward_send,
    inward_recv,
    early_send,
    early_recv,
    cross_send,
    near_send,
    near_recv,
    far_send,
    far_recv,
    relay_send,
    relay_recv,
):
    states, held = (state0, state1, state2), (held0, held1, held2)
    rank = lax.axis_index("dp")
    place = lax.axis_index("tensor")
    row, core = rank // 2, rank % 2
    near = row * 2 + 1 - core
    far = (1 - row) * 2 + core
    across = (1 - row) * 2 + 1 - core
    subs = land.shape[1]
    slab = mine.shape[0]
    width = land.shape[4]
    chunk = CHUNK
    steps = slab // chunk
    owner, sub = place // subs, place % subs
    side, owner_core = owner // 2, owner % 2
    group = 2 * subs
    span = group * width
    home = row == side
    away = row != side
    same_cols = pl.ds(pl.multiple_of(side * span, span), span)
    apart_cols = pl.ds(pl.multiple_of((1 - side) * span, span), span)
    slot = jnp.where(home, 0, 1)

    def rows(step):
        return pl.ds(pl.multiple_of(step * chunk, chunk), chunk)

    def columns(goal):
        return pl.ds(pl.multiple_of(goal * width, width), width)

    def remote(source, target, send, recv, to_rank, to_place):
        return pltpu.make_async_remote_copy(
            src_ref=source,
            dst_ref=target,
            send_sem=send,
            recv_sem=recv,
            device_id=(to_rank, to_place),
            device_id_type=MESH,
        )

    def arrived(spot, sem):
        pltpu.make_async_copy(spot, spot, sem).wait()

    ready = READY * chunk
    stops = (*(stop for stop in SWAPS if stop < steps), steps)
    pieces = tuple(zip((0, *stops[:-1]), stops))
    late = steps - PRE
    kept = pl.ds(0, late * chunk)
    tail = pl.ds(late * chunk, PRE * chunk)

    def load(which):
        part = pl.ds(0, ready) if which == 0 else pl.ds(ready, slab - ready)
        return pltpu.make_async_copy(
            grads.at[0, core, part], mine.at[part], load_sem.at[which]
        )

    def bring():
        part = pl.ds(0, ready)
        return pltpu.make_async_copy(grads.at[0, 1 - core, part], leaving, load_sem.at[2])

    def swap(piece):
        start, stop = pieces[piece]
        part = pl.ds(start * chunk, (stop - start) * chunk)
        source = leaving.at[part] if stop <= READY else grads.at[0, 1 - core, part]
        return remote(source, theirs.at[part], swap_send, swap_recv.at[piece], near, place)

    def state(which):
        return pltpu.make_async_copy(states[which], held[which], state_sem.at[which])

    def inbound(step):
        return remote(
            mine.at[rows(step), same_cols], inward.at[rows(step)],
            inward_send, inward_recv.at[step], far, place,
        )

    def forward():
        return remote(
            mine.at[tail, apart_cols], early, early_send, early_recv, far, place
        )

    def spread_apart(step, offset):
        goal = (1 - side) * group + (place + offset) % group
        return remote(
            mine.at[rows(step), columns(goal)],
            land.at[slot, sub, core, rows(step)],
            apart_send,
            land_recv.at[step],
            row * 2 + owner_core,
            goal,
        )

    def spread_same(step, offset):
        goal = side * group + (place + offset) % group
        return remote(
            mine.at[rows(step), columns(goal)],
            land.at[0, sub, core, rows(step)],
            same_send,
            land_recv.at[step],
            row * 2 + owner_core,
            goal,
        )

    def spread_self(step):
        return pltpu.make_async_copy(
            mine.at[rows(step), columns(place)],
            land.at[0, sub, core, rows(step)],
            land_recv.at[step],
        )

    def landed(step):
        arrived(land.at[:, :, :, rows(step)], land_recv.at[step])

    def landed_own(step):
        arrived(land.at[0, :, :, rows(step)], land_recv.at[step])

    def cross(step):
        return remote(
            land.at[1, :, :, rows(step)], land.at[1, :, :, rows(step)],
            cross_send, land_recv.at[step], far, place,
        )

    def block(of_rank, step):
        return roll.at[:, pl.ds(of_rank * subs, subs), rows(step)]

    def to_near(of_rank, step):
        return remote(
            block(of_rank, step), block(of_rank, step),
            near_send, near_recv, near, place,
        )

    def to_far(of_rank, step):
        return remote(
            block(of_rank, step), block(of_rank, step),
            far_send, far_recv.at[step], far, place,
        )

    def relay(of_rank, step):
        return remote(
            block(of_rank, step), block(of_rank, step),
            relay_send, relay_recv, near, place,
        )

    def combine(step, cols, third=None, base=0):
        @pl.loop(0, chunk // STRIP)
        def _(i):
            at = pl.ds(pl.multiple_of(step * chunk + i * STRIP, STRIP), STRIP)
            total = mine[at, cols].astype(jnp.float32) + theirs[at, cols].astype(jnp.float32)
            if third is not None:
                place_of = (step - base) * chunk + i * STRIP
                total = total + third[pl.ds(pl.multiple_of(place_of, STRIP), STRIP)].astype(
                    jnp.float32
                )
            mine[at, cols] = total.astype(mine.dtype)

    def issue_inward(step):
        combine(step, same_cols)
        inbound(step).start()

    def issue_apart(step):
        for offset in range(group):
            spread_apart(step, offset).start()

    def issue_same(step):
        inbound(step).wait_recv()
        combine(step, same_cols, inward)
        for offset in range(1, group):
            spread_same(step, offset).start()

        @pl.when(owner_core == core)
        def _():
            spread_self(step).start()

        @pl.when(owner_core != core)
        def _():
            spread_same(step, 0).start()

    def pass_on(step):
        to_far(far, step).wait_recv()
        relay(far, step).start()

    last = steps + LATE
    first_fix = 1.0 - 0.9**10
    second_fix = 1.0 - 0.95**10

    def update(step, crossed):
        @pl.loop(0, chunk // STRIP)
        def _(i):
            at = pl.ds(pl.multiple_of(step * chunk + i * STRIP, STRIP), STRIP)
            for half in range(2):
                for piece in range(subs):
                    grad = land[0, piece, half, at].astype(jnp.float32)
                    if crossed:
                        grad = grad + land[1, piece, half, at].astype(jnp.float32)
                    old = held[0][half, piece, at]
                    moment1 = 0.9 * held[1][half, piece, at] + 0.1 * grad
                    moment2 = 0.95 * held[2][half, piece, at] + 0.05 * grad * grad
                    scaled = jnp.sqrt(moment2 * (1.0 / second_fix)) + 1e-08
                    change = moment1 * (1.0 / first_fix) / scaled + 0.1 * old
                    new = old - 0.003 * change
                    held[0][half, piece, at] = new
                    held[1][half, piece, at] = moment1
                    held[2][half, piece, at] = moment2
                    roll[half, rank * subs + piece, at] = new.astype(roll.dtype)

        to_far(rank, step).start()
        to_near(rank, step).start()

    barrier = pltpu.get_barrier_semaphore()
    peers = 0
    for hop in range(tensor_count):
        goal = (place + hop) % tensor_count
        for which in range(2):
            if hop or which:
                pl.semaphore_signal(
                    barrier, inc=1, device_id=(row * 2 + (core + which) % 2, goal), device_id_type=MESH
                )
                peers += 1
    pl.semaphore_signal(barrier, inc=1, device_id=(far, place), device_id_type=MESH)
    peers += 1

    load(0).start()
    bring().start()
    token_copy = pltpu.make_async_copy(tokens, token_rows, token_sem)
    table_copy = pltpu.make_async_copy(route, table, table_sem)
    table_copy.start()
    wide = tensor_count * LANES
    picks = token_rows.shape[1] // wide

    def pick(part):
        at = pl.ds(pl.multiple_of(part * wide, wide), wide)
        some = jnp.dot(chosen[...], token_rows[:, at], preferred_element_type=jnp.float32)
        picked[:, at] = some.astype(picked.dtype)

    def pick_now(now):
        @pl.when(now == PICK)
        def _():
            token_copy.wait()
            table_copy.wait()
            index = lax.broadcasted_iota(jnp.int32, (token_rows.shape[0], table.shape[1]), 0)
            onehot = jnp.where(index == table[...], 1.0, 0.0)
            chosen[...] = onehot.T.astype(chosen.dtype)

        @pl.when((now >= PICK) & (now < PICK + picks))
        def _():
            pick(now - PICK)

    load(0).wait()
    bring().wait()
    pl.semaphore_wait(barrier, peers)
    for piece in range(len(pieces)):
        swap(piece).start()
    load(1).start()
    for which in range(3):
        state(which).start()
    token_copy.start()

    def first(step, action):
        for piece, (start, _) in enumerate(pieces):
            if start == step:
                swap(piece).wait_recv()
        if step == READY:
            load(1).wait()
        action(step)

    def rest(begin):
        for piece, (start, _) in enumerate(pieces):
            if start >= begin:
                swap(piece).wait_recv()
        if begin <= READY:
            load(1).wait()
        for which in range(3):
            state(which).wait()

    def apart_plain(step):
        combine(step, apart_cols)
        issue_apart(step)

    @pl.when(home)
    def _():
        for step in range(AHEAD):
            first(step, apart_plain)
        for step in range(SAME):
            issue_same(step)
        rest(AHEAD)

        @pl.loop(0, last)
        def _(now):
            @pl.when(now < late)
            def _():
                landed(now)
                cross(now).start()

            @pl.when(now < late - AHEAD)
            def _():
                apart_plain(now + AHEAD)

            @pl.when(now == late - AHEAD)
            def _():
                forward().wait_recv()

            @pl.when((now >= late - AHEAD) & (now < steps - AHEAD))
            def _():
                combine(now + AHEAD, apart_cols, early, late)
                issue_apart(now + AHEAD)

            @pl.when(now < steps - SAME)
            def _():
                issue_same(now + SAME)

            @pl.when(now >= LATE)
            def _():
                pass_on(now - LATE)

            @pl.when((now >= late) & (now < steps))
            def _():
                landed_own(now)

            @pl.when(now < steps)
            def _():
                update(now, False)

            pick_now(now)

    @pl.when(away)
    def _():
        def both(step):
            issue_inward(step)
            apart_plain(step)

        for step in range(AHEAD):
            first(step, both)
        for step in range(AHEAD, LEAD):
            first(step, issue_inward)
        rest(LEAD)

        @pl.loop(late, steps)
        def _(step):
            combine(step, apart_cols)

        forward().start()

        @pl.loop(0, last)
        def _(now):
            @pl.when(now < late - AHEAD)
            def _():
                apart_plain(now + AHEAD)

            @pl.when(now < steps - LEAD)
            def _():
                issue_inward(now + LEAD)

            @pl.when(now < late)
            def _():
                landed(now)
                update(now, True)

            @pl.when((now >= late) & (now < steps))
            def _():
                landed_own(now)
                update(now, False)

            @pl.when(now >= LATE)
            def _():
                pass_on(now - LATE)

            pick_now(now)

    arrived(theirs, swap_send)

    @pl.when(away)
    def _():
        arrived(mine.at[kept, apart_cols], apart_send)
        arrived(inward, inward_send)
        forward().wait_send()

    @pl.when(home)
    def _():
        arrived(mine.at[:, apart_cols], apart_send)
        arrived(land.at[1, :, :, kept], cross_send)

    @pl.when(home & (owner_core == core))
    def _():
        arrived(mine.at[:, pl.ds(0, span - width)], same_send)

    @pl.when(home & (owner_core != core))
    def _():
        arrived(mine.at[:, pl.ds(0, span)], same_send)

    own = roll.at[:, pl.ds(rank * subs, subs)]
    arrived(own, far_send)
    arrived(own, near_send)
    arrived(own, relay_send)
    arrived(roll.at[:, pl.ds(near * subs, subs)], near_recv)
    arrived(roll.at[:, pl.ds(across * subs, subs)], relay_recv)


def finish_kernel(
    held0, held1, held2, roll, picked, out0, out1, out2, full, hidden, acc, small, sems
):
    copies = []
    for source, target in ((held0, out0), (held1, out1), (held2, out2), (roll, full)):
        for half in range(2):
            size = source.shape[1] // 4
            for part in range(4):
                at = pl.ds(part * size, size)
                copies.append(
                    pltpu.make_async_copy(
                        source.at[half, at], target.at[half, at], sems.at[len(copies)]
                    )
                )
    for copy in copies:
        copy.start()
    acc[...] = jnp.zeros_like(acc)
    depth = picked.shape[1]
    wide = depth // 7 if depth % (7 * LANES) == 0 else LANES

    @pl.loop(0, depth // wide)
    def _(part):
        at = pl.ds(pl.multiple_of(part * wide, wide), wide)
        for half in range(2):
            acc[half] += jnp.dot(
                picked[:, at], roll[half, at], preferred_element_type=jnp.float32
            )

    gate, up = acc[0], acc[1]
    small[...] = (gate / (1.0 + jnp.exp(-gate)) * up).astype(small.dtype)
    last = pltpu.make_async_copy(small, hidden, sems.at[len(copies)])
    last.start()
    for copy in copies:
        copy.wait()
    last.wait()


def fused(grads, master, moment1, moment2, tokens, route):
    tensor_count = lax.axis_size("tensor")
    rank_count = lax.axis_size("dp")
    subs = tensor_count // rank_count
    slab, hidden_width = grads.shape[2:]
    width = hidden_width // tensor_count
    steps = slab // CHUNK
    routed = route.shape[0]
    depth = tokens.shape[1]
    split = (2, subs, slab, width)
    states = [array.reshape(split) for array in (master, moment1, moment2)]
    anywhere = pl.BlockSpec(memory_space=pl.ANY)
    vmem = pl.BlockSpec(memory_space=pltpu.VMEM)
    hbm = pl.BlockSpec(memory_space=pltpu.HBM)
    dma = pltpu.SemaphoreType.DMA
    half = jnp.bfloat16
    f32 = jnp.float32
    parts = pl.pallas_call(
        functools.partial(reduce_kernel, tensor_count),
        out_shape=[pltpu.VMEM(split, f32)] * 3
        + [
            pltpu.VMEM((2, tensor_count, slab, width), half),
            pltpu.VMEM((routed, depth), half),
        ],
        in_specs=[anywhere] * 6,
        out_specs=[vmem] * 5,
        scratch_shapes=[
            pltpu.VMEM((slab, hidden_width), half),
            pltpu.VMEM((slab, hidden_width), half),
            pltpu.VMEM((READY * CHUNK, hidden_width), half),
            pltpu.VMEM((2, subs, 2, slab, width), half),
            pltpu.VMEM((slab, hidden_width // 2), half),
            pltpu.VMEM((PRE * CHUNK, hidden_width // 2), half),
            pltpu.VMEM(tokens.shape, half),
            pltpu.VMEM((routed, tokens.shape[0]), half),
            pltpu.VMEM((1, routed), jnp.int32),
            dma((3,)),
            dma,
            dma((len(SWAPS) + 1,)),
            dma((3,)),
            dma,
            dma,
            dma,
            dma,
            dma((steps,)),
            dma,
            dma((steps,)),
            dma,
            dma,
            dma,
            dma,
            dma,
            dma,
            dma((steps,)),
            dma,
            dma,
        ],
        compiler_params=pltpu.CompilerParams(
            has_side_effects=True, collective_id=0, vmem_limit_bytes=42 * 1024 * 1024
        ),
    )(grads, *states, tokens, route.reshape(1, routed))
    whole = (2, subs * slab, width)
    wide = (2, tensor_count * slab, width)
    *held, roll, picked = parts
    held = [array.reshape(whole) for array in held]
    new_master, new1, new2, rollout, hidden = pl.pallas_call(
        finish_kernel,
        out_shape=[pltpu.HBM(whole, f32)] * 3
        + [pltpu.HBM(wide, half), pltpu.HBM((routed, width), half)],
        in_specs=[vmem] * 5,
        out_specs=[hbm] * 5,
        scratch_shapes=[
            pltpu.VMEM((2, routed, width), f32),
            pltpu.VMEM((routed, width), half),
            dma((33,)),
        ],
        compiler_params=pltpu.CompilerParams(vmem_limit_bytes=8 * 1024 * 1024),
    )(*held, roll.reshape(wide), picked)
    return (new_master, new1, new2, rollout, hidden)


def chosen_body(grads, master, moment1, moment2, tokens, route):
    tensor_count, rank_count = lax.axis_size("tensor"), lax.axis_size("dp")
    slab, hidden_width = grads.shape[2:]
    fits = (
        rank_count == 4
        and tensor_count % rank_count == 0
        and slab % LANES == 0
        and slab % CHUNK == 0
        and slab // CHUNK > max(LEAD, *SWAPS, AHEAD + PRE)
        and tokens.shape[1] // (tensor_count * LANES) + PICK <= slab // CHUNK
        and tokens.shape[1] % (tensor_count * LANES) == 0
        and hidden_width % (tensor_count * LANES) == 0
    )
    chosen = fused if fits else body
    return chosen(grads, master, moment1, moment2, tokens, route)


def solution(mesh):
    in_specs = (
        P("dp", None, "tensor", None),
        P(None, "dp", "tensor"),
        P(None, "dp", "tensor"),
        P(None, "dp", "tensor"),
        P("dp", None),
        P("dp"),
    )
    out_specs = (
        P(None, "dp", "tensor"),
        P(None, "dp", "tensor"),
        P(None, "dp", "tensor"),
        P(None, None, "tensor"),
        P("dp", "tensor"),
    )
    return jax.shard_map(chosen_body, mesh=mesh, in_specs=in_specs, out_specs=out_specs, check_vma=False)
```
